128 devices in a mesh: blk: 64 (over x_lo, y, z, core), tensor: 2 (over x_hi).
Axes of the slice: x: 4 (x_hi: 2, x_lo: 2; x = x_hi * 2 + x_lo), y: 4, z: 4, core: 2. Of those that a mesh axis runs over, the one named last changes fastest.
Arguments:
- tokens: bfloat16 [256, 8192], P('blk'), may hold values from -6 to 6
- gate_weight: bfloat16 [29568, 8192], P(('blk', 'tensor')), may hold values from -0.0625 to 0.0625
- up_weight: bfloat16 [29568, 8192], P(('blk', 'tensor')), may hold values from -0.0625 to 0.0625
- down_weight: bfloat16 [29568, 8192], P(('blk', 'tensor')), may hold values from -0.03125 to 0.03125
Outputs:
- mixed: bfloat16 [256, 8192], P(('blk', 'tensor'))
The draws below stay inside these ranges and needn't reach their ends.
All inputs are finite; a program needn't handle non-finite values.
Results may differ from the reference program's by a relative error of at most 0.009.
Values may be sent and summed in bfloat16 or wider, within the bound.
A program may use at most 64 MiB of HBM per device.

```python
import jax
import jax.numpy as jnp

D = 8192
FF = 29568
TOKENS = 256


def level_of(own_key, extent, shards, low, high):
    factor_of, own = 1.0, jax.random.fold_in(own_key, 6)
    for axis_at, shards_of in shards:
        draws = jnp.exp(jax.random.uniform(jax.random.fold_in(own, axis_at), (shards_of,), jnp.float32, low / len(shards), high / len(shards)))
        factor_of = factor_of * jnp.repeat(draws, extent[axis_at] // shards_of).reshape([-1 if axis == axis_at else 1 for axis in range(len(extent))])
    return factor_of


def bell_draw(own_key, extent, width, most, pieces=(), kind=jnp.bfloat16):
    level = level_of(own_key, extent, pieces, -0.22, 0.18) if pieces else 1.0
    result = jax.random.normal(own_key, extent, jnp.float32) * width * level
    return jnp.minimum(jnp.maximum(result, -most), most).astype(kind)


def setup_inputs(seed: int = 0) -> dict:
    key_of = jax.random.split(jax.random.key(seed), 5)
    tokens = bell_draw(key_of[0], (TOKENS, D), 1.0, 6.0, ((0, 64),))
    gate_weight = bell_draw(key_of[1], (FF, D), D ** -0.5, 0.0625, ((0, 128),))
    up_weight = bell_draw(key_of[2], (FF, D), D ** -0.5, 0.0625, ((0, 128),))
    down_weight = bell_draw(key_of[3], (FF, D), FF ** -0.5, 0.03125, ((0, 128),))
    return {"tokens": tokens, "gate_weight": gate_weight, "up_weight": up_weight, "down_weight": down_weight}


def reference(tokens, gate_weight, up_weight, down_weight):
    gate = jnp.dot(tokens, gate_weight.T, preferred_element_type=jnp.float32)
    up = jnp.dot(tokens, up_weight.T, preferred_element_type=jnp.float32)
    hidden = (jax.nn.silu(gate) * up).astype(jnp.bfloat16)
    return jnp.dot(hidden, down_weight, preferred_element_type=jnp.float32).astype(jnp.bfloat16)
```

```python
import jax
import jax.numpy as jnp
from jax import lax
from jax.experimental import pallas as pl
from jax.experimental.pallas import tpu as pltpu
from jax.sharding import PartitionSpec as P

F32 = jnp.float32
BF16 = jnp.bfloat16
MESH = pl.DeviceIdType.MESH
D = 8192
HALF = D // 2
TOKENS = 256

CHUNK_TILES = ((8, 7, 7), (7, 7, 7), (7, 7, 7))
ORDERS = ("xyz", "yzx", "zxy")


def chunks_of():
    chunks, start = [[], [], []], 0
    for colour, tiles in enumerate(CHUNK_TILES):
        for tile in tiles:
            chunks[colour].append((colour, start * 128, tile * 128, (tile + 1) // 2 * 128))
            start += tile
    return [chunks[colour][at] for at in range(3) for colour in range(3)]


CHUNKS = chunks_of()
NC = len(CHUNKS)
N_GATHER = 96
N_RS = 13 * NC


def kernel(
    tokens_hbm, gate_hbm, up_hbm, down_hbm, out_ref,
    own4, recv4, tok, gate_w, up_w, down_w, own, d2d_send, d2d_recv,
    sa, rl, rp, rm, sb, rb, sc, rc,
    local_sem, g_send, g_recv, r_send, r_recv,
):
    blk = lax.axis_index("blk")
    x_hi = lax.axis_index("tensor")
    core = blk % 2
    z = (blk // 2) % 4
    y = (blk // 8) % 4
    x_lo = blk // 32
    x = x_hi * 2 + x_lo
    at = {"x": x, "y": y, "z": z}

    def device(dx=0, dy=0, dz=0, dcore=0):
        tx, ty, tz = (x + dx + 4) % 4, (y + dy + 4) % 4, (z + dz + 4) % 4
        tc = (core + dcore) % 2
        return {"blk": (((tx % 2) * 4 + ty) * 4 + tz) * 2 + tc, "tensor": tx // 2}

    def shifted(axis, delta):
        return device(**{"d" + axis: delta})

    partner = device(dcore=1)

    load_tokens = pltpu.make_async_copy(tokens_hbm, own4, local_sem.at[0])
    load_tokens.start()
    loads = [
        pltpu.make_async_copy(src, dst, local_sem.at[1 + i])
        for i, (src, dst) in enumerate(((gate_hbm, gate_w), (up_hbm, up_w), (down_hbm, down_w)))
    ]
    for load in loads:
        load.start()

    barrier = pltpu.get_barrier_semaphore()
    peers = [partner] + [shifted(axis, delta) for axis in "xyz" for delta in (1, 2, 3)]
    for peer in peers:
        pl.semaphore_signal(barrier, inc=1, device_id=peer, device_id_type=MESH)
    pl.semaphore_wait(barrier, len(peers))

    sends = []
    counter = [0]

    def new_sem():
        counter[0] += 1
        return counter[0] - 1

    def send(src, dst, sem, to, pool=None):
        s, r = pool or (g_send, g_recv)
        copy = pltpu.make_async_remote_copy(
            src_ref=src, dst_ref=dst, send_sem=s.at[sem], recv_sem=r.at[sem],
            device_id=to, device_id_type=MESH,
        )
        copy.start()
        sends.append(copy)

    def arrived(ref, sem, pool=None):
        s, r = pool or (g_send, g_recv)
        pltpu.make_async_remote_copy(
            src_ref=ref, dst_ref=ref, send_sem=s.at[sem], recv_sem=r.at[sem],
            device_id=partner, device_id_type=MESH,
        ).wait_recv()

    load_tokens.wait()
    mine = pl.multiple_of(core * HALF, HALF)
    theirs = pl.multiple_of((1 - core) * HALF, HALF)
    sem = new_sem()
    send(own4.at[:, pl.ds(theirs, HALF)], recv4, sem, partner)
    arrived(recv4, sem)
    a = own4[:, pl.ds(mine, HALF)].astype(F32)
    b = recv4[...].astype(F32)
    first = core == 0
    unit = jnp.concatenate([jnp.where(first, a, b), jnp.where(first, b, a)], axis=0)
    tok[x_lo, y, z, :, pl.ds(mine, HALF)] = unit.astype(BF16)

    Q = HALF // 4
    H = Q // 2

    def cols(colour, part=None, base=None):
        base = mine if base is None else base
        if part is None:
            return pl.ds(pl.multiple_of(base + colour * Q, 128), Q)
        return pl.ds(pl.multiple_of(base + colour * Q + part * H, 128), H)

    def piece(xl, yy, zz, c):
        return tok.at[xl, yy, zz, :, c]

    everything = slice(None)
    other = 1 - x_lo

    def line(colour, first_axis, fixed, c, xl):
        if first_axis == "y":
            return tok.at[xl, :, fixed, :, c]
        return tok.at[xl, fixed, :, :, c]

    d2d_sems = []

    def forward(make_ref):
        sem = new_sem()
        ref = make_ref(mine)
        send(ref, ref, sem, partner)
        d2d_sems.append((sem, make_ref))

    axes = {0: ("y", "z"), 1: ("z", "y"), 2: ("z", "y"), 3: ("y", "z")}

    s1 = {}
    for colour in range(4):
        p, q = axes[colour]
        for delta in (1, 3, 2):
            s1[colour, delta] = new_sem()
            ref = piece(x_lo, y, z, cols(colour))
            send(ref, ref, s1[colour, delta], shifted(p, delta))

    xs, qs, ring = {}, {}, {}

    def both_x(colour, fixed, key):
        p, q = axes[colour]
        for part, delta in ((0, 1), (1, 3)):
            xs[colour, key, part] = new_sem()
            ref = line(colour, p, fixed, cols(colour, part), x_lo)
            send(ref, ref, xs[colour, key, part], shifted("x", delta))

    def start_ring(colour, xl, key):
        p, q = axes[colour]
        for delta in (1, 3):
            ring[colour, key, delta] = new_sem()
            ref = line(colour, p, at[q], cols(colour), xl)
            send(ref, ref, ring[colour, key, delta], shifted(q, delta))

    def pass_ring(colour, xl, key, delta):
        p, q = axes[colour]
        place = (at[q] - delta + 4) % 4
        ref = line(colour, p, place, cols(colour), xl)
        arrived(ref, ring[colour, key, delta])
        part = 0 if delta == 1 else 1
        ring[colour, key, delta, "far"] = new_sem()
        ref = line(colour, p, place, cols(colour, part), xl)
        send(ref, ref, ring[colour, key, delta, "far"], shifted(q, delta))
        return place

    def end_ring(colour, xl, key, delta):
        p, q = axes[colour]
        place = (at[q] + 2) % 4
        part = 0 if delta == 1 else 1
        arrived(line(colour, p, place, cols(colour, part), xl), ring[colour, key, delta, "far"])
        return place

    def forward_line(colour, fixed, xl):
        p, _ = axes[colour]
        forward(lambda base: line(colour, p, fixed, cols(colour, None, base), xl))

    for colour in range(4):
        p, q = axes[colour]
        for delta in (1, 3, 2):
            place = {p: (at[p] - delta + 4) % 4, q: at[q]}
            arrived(piece(x_lo, place["y"], place["z"], cols(colour)), s1[colour, delta])
        if colour < 2:
            start_ring(colour, x_lo, "own")
            both_x(colour, at[q], 0)
        else:
            both_x(colour, at[q], 0)
            start_ring(colour, x_lo, "own")
        forward_line(colour, at[q], x_lo)

    for colour in (0, 1):
        for delta in (1, 3):
            place = pass_ring(colour, x_lo, "own", delta)
            both_x(colour, place, delta)
            forward_line(colour, place, x_lo)
    for colour in (2, 3):
        p, q = axes[colour]
        for part in (0, 1):
            arrived(line(colour, p, at[q], cols(colour, part), other), xs[colour, 0, part])
        start_ring(colour, other, "other")
        forward_line(colour, at[q], other)
    for colour in (2, 3):
        for delta in (1, 3):
            place = pass_ring(colour, x_lo, "own", delta)
            forward_line(colour, place, x_lo)

    for colour in (0, 1):
        p, q = axes[colour]
        place = (at[q] + 2) % 4
        for delta, part, step in ((1, 0, 1), (3, 1, 3)):
            end_ring(colour, x_lo, "own", delta)
            xs[colour, 2, part] = new_sem()
            ref = line(colour, p, place, cols(colour, part), x_lo)
            send(ref, ref, xs[colour, 2, part], shifted("x", step))
        forward_line(colour, place, x_lo)
        for key in (0, 1, 3):
            place = (at[q] - key + 4) % 4
            for part in (0, 1):
                arrived(line(colour, p, place, cols(colour, part), other), xs[colour, key, part])
            forward_line(colour, place, other)
    for colour in (2, 3):
        for delta in (1, 3):
            place = pass_ring(colour, other, "other", delta)
            forward_line(colour, place, other)
    for colour in (2, 3):
        for delta in (1, 3):
            place = end_ring(colour, x_lo, "own", delta)
        forward_line(colour, place, x_lo)

    for colour in (0, 1):
        p, q = axes[colour]
        place = (at[q] + 2) % 4
        for part in (0, 1):
            arrived(line(colour, p, place, cols(colour, part), other), xs[colour, 2, part])
        forward_line(colour, place, other)
    for colour in (2, 3):
        for delta in (1, 3):
            place = end_ring(colour, other, "other", delta)
        forward_line(colour, place, other)

    for load in loads[:2]:
        load.wait()
    flat = tok.reshape(TOKENS, D)

    def project(weight, base):
        return lax.dot_general(
            flat[:, pl.ds(base, HALF)], weight[:, pl.ds(base, HALF)],
            (((1,), (1,)), ((), ())), preferred_element_type=F32,
        )

    gate = project(gate_w, mine)
    up = project(up_w, mine)
    for sem, make_ref in d2d_sems:
        arrived(make_ref(theirs), sem)
    gate = gate + project(gate_w, theirs)
    up = up + project(up_w, theirs)
    hidden = (gate / (1.0 + jnp.exp(-gate)) * up).astype(BF16)

    rho = lax.broadcasted_iota(jnp.int32, (TOKENS, TOKENS), 0)
    token = lax.broadcasted_iota(jnp.int32, (TOKENS, TOKENS), 1)
    t_core = (rho // 128 + core) % 2
    hiddens = []
    for order in ORDERS:
        where = {}
        for axis, width in zip(order, (32, 8, 2)):
            where[axis] = ((rho // width) % 4 + at[axis]) % 4
        t_blk = (((where["x"] % 2) * 4 + where["y"]) * 4 + where["z"]) * 2 + t_core
        t_row = t_blk * 4 + (where["x"] // 2) * 2 + rho % 2
        pick = jnp.where(t_row == token, 1.0, 0.0).astype(BF16)
        hiddens.append(jnp.dot(pick, hidden, preferred_element_type=F32).astype(BF16))

    pool = (r_send, r_recv)
    loads[2].wait()
    for i, (colour, start, width, left) in enumerate(CHUNKS):
        c = pl.ds(start, width)
        part = jnp.dot(hiddens[colour], down_w[:, c], preferred_element_type=F32)
        d2d_send[:, c] = part[128:].astype(BF16)
        own[:, c] = part[:128]
        send(d2d_send.at[:, c], d2d_recv.at[:, c], i * 13, partner, pool)

    for i, (colour, start, width, left) in enumerate(CHUNKS):
        axis = ORDERS[colour][0]
        c, cl, cr = pl.ds(start, width), pl.ds(start, left), pl.ds(start + left, width - left)
        arrived(d2d_recv.at[:, c], i * 13, pool)
        sa[64:96, c] = (own[64:96, c] + d2d_recv[64:96, c].astype(F32)).astype(BF16)
        send(sa.at[64:96, cl], rl.at[:, cl], i * 13 + 1, shifted(axis, 1), pool)
        send(sa.at[64:96, cr], rl.at[:, cr], i * 13 + 2, shifted(axis, 3), pool)
        sa[32:64, cr] = (own[32:64, cr] + d2d_recv[32:64, cr].astype(F32)).astype(BF16)
        send(sa.at[32:64, cr], rp.at[:, cr], i * 13 + 3, shifted(axis, 1), pool)
        sa[96:128, cl] = (own[96:128, cl] + d2d_recv[96:128, cl].astype(F32)).astype(BF16)
        send(sa.at[96:128, cl], rm.at[:, cl], i * 13 + 4, shifted(axis, 3), pool)
    for i, (colour, start, width, left) in enumerate(CHUNKS):
        axis = ORDERS[colour][0]
        c, cl, cr = pl.ds(start, width), pl.ds(start, left), pl.ds(start + left, width - left)
        arrived(rl.at[:, cl], i * 13 + 1, pool)
        sa[32:64, cl] = (
            own[32:64, cl] + d2d_recv[32:64, cl].astype(F32) + rl[:, cl].astype(F32)
        ).astype(BF16)
        send(sa.at[32:64, cl], rp.at[:, cl], i * 13 + 5, shifted(axis, 1), pool)
        arrived(rl.at[:, cr], i * 13 + 2, pool)
        sa[96:128, cr] = (
            own[96:128, cr] + d2d_recv[96:128, cr].astype(F32) + rl[:, cr].astype(F32)
        ).astype(BF16)
        send(sa.at[96:128, cr], rm.at[:, cr], i * 13 + 6, shifted(axis, 3), pool)

    for i, (colour, start, width, left) in enumerate(CHUNKS):
        axis = ORDERS[colour][1]
        c, cl, cr = pl.ds(start, width), pl.ds(start, left), pl.ds(start + left, width - left)
        arrived(rp.at[:, cr], i * 13 + 3, pool)
        arrived(rm.at[:, cl], i * 13 + 4, pool)
        arrived(rp.at[:, cl], i * 13 + 5, pool)
        arrived(rm.at[:, cr], i * 13 + 6, pool)
        total = (
            own[0:32, c] + d2d_recv[0:32, c].astype(F32)
            + rp[:, c].astype(F32) + rm[:, c].astype(F32)
        )
        own[0:8, c] = total[0:8]
        for delta in (2, 1, 3):
            sb[delta, :, c] = total[delta * 8:delta * 8 + 8].astype(BF16)
            send(sb.at[delta, :, c], rb.at[delta, :, c], i * 13 + 6 + delta, shifted(axis, delta), pool)

    for i, (colour, start, width, left) in enumerate(CHUNKS):
        axis = ORDERS[colour][2]
        c = pl.ds(start, width)
        total = own[0:8, c]
        for delta in (1, 3, 2):
            arrived(rb.at[delta, :, c], i * 13 + 6 + delta, pool)
            total = total + rb[delta, :, c].astype(F32)
        own[0:8, c] = total
        for delta in (2, 1, 3):
            sc[delta, :, c] = total[delta * 2:delta * 2 + 2].astype(BF16)
            send(sc.at[delta, :, c], rc.at[delta, :, c], i * 13 + 9 + delta, shifted(axis, delta), pool)
    for i, (colour, start, width, left) in enumerate(CHUNKS):
        c = pl.ds(start, width)
        total = own[0:2, c]
        for delta in (1, 3, 2):
            arrived(rc.at[delta, :, c], i * 13 + 9 + delta, pool)
            total = total + rc[delta, :, c].astype(F32)
        out_ref[:, c] = total.astype(BF16)

    for copy in sends:
        copy.wait_send()
    assert counter[0] <= N_GATHER


def per_device(tokens, gate_weight, up_weight, down_weight):
    hidden = gate_weight.shape[0]
    return pl.pallas_call(
        kernel,
        out_shape=jax.ShapeDtypeStruct((2, D), BF16),
        in_specs=[pl.BlockSpec(memory_space=pl.ANY)] * 4,
        out_specs=pl.BlockSpec(memory_space=pltpu.VMEM),
        scratch_shapes=[
            pltpu.VMEM((4, D), BF16),
            pltpu.VMEM((4, HALF), BF16),
            pltpu.VMEM((2, 4, 4, 8, D), BF16),
            pltpu.VMEM((hidden, D), BF16),
            pltpu.VMEM((hidden, D), BF16),
            pltpu.VMEM((hidden, D), BF16),
            pltpu.VMEM((128, D), F32),
            pltpu.VMEM((128, D), BF16),
            pltpu.VMEM((128, D), BF16),
            pltpu.VMEM((128, D), BF16),
            pltpu.VMEM((32, D), BF16),
            pltpu.VMEM((32, D), BF16),
            pltpu.VMEM((32, D), BF16),
            pltpu.VMEM((4, 8, D), BF16),
            pltpu.VMEM((4, 8, D), BF16),
            pltpu.VMEM((4, 2, D), BF16),
            pltpu.VMEM((4, 2, D), BF16),
            pltpu.SemaphoreType.DMA((4,)),
            pltpu.SemaphoreType.DMA((N_GATHER,)),
            pltpu.SemaphoreType.DMA((N_GATHER,)),
            pltpu.SemaphoreType.DMA((N_RS,)),
            pltpu.SemaphoreType.DMA((N_RS,)),
        ],
        compiler_params=pltpu.CompilerParams(
            collective_id=0, has_side_effects=True, vmem_limit_bytes=63 * 1024 * 1024
        ),
    )(tokens, gate_weight, up_weight, down_weight)


def solution(mesh):
    placed = (
        P("blk", None),
        P(("blk", "tensor"), None),
        P(("blk", "tensor"), None),
        P(("blk", "tensor"), None),
    )
    return jax.shard_map(
        per_device,
        mesh=mesh,
        in_specs=placed,
        out_specs=P(("blk", "tensor"), None),
        check_vma=False,
    )
```
